8 devices in a mesh: dp: 1 (over z), ep: 8 (over y, x, core).
Axes of the slice: x: 2, y: 2, z: 1, core: 2. Of those that a mesh axis runs over, the one named last changes fastest.
Arguments:
- tokens_a: bfloat16 [256, 1536], P(('dp', 'ep'))
- experts_a: int32 [256, 8], P(('dp', 'ep'))
- slots_a: int32 [256, 8], P(('dp', 'ep'))
- gates_a: bfloat16 [256, 8], P(('dp', 'ep'))
- tokens_b: bfloat16 [256, 1536], P(('dp', 'ep'))
- experts_b: int32 [256, 8], P(('dp', 'ep'))
- slots_b: int32 [256, 8], P(('dp', 'ep'))
- gates_b: bfloat16 [256, 8], P(('dp', 'ep'))
- attn_gain: bfloat16 [1536], replicated
- w_query: bfloat16 [1536, 24, 64], replicated
- w_key: bfloat16 [1536, 24, 64], replicated
- w_value: bfloat16 [1536, 24, 64], replicated
- w_out: bfloat16 [24, 64, 1536], replicated
- moe_gain: bfloat16 [1536], replicated
- w_gate: bfloat16 [40, 1536, 512], P('ep')
- w_up: bfloat16 [40, 1536, 512], P('ep')
- w_down: bfloat16 [40, 512, 1536], P('ep')
Outputs:
- output 1: bfloat16 [256, 1536], P(('dp', 'ep'))
- output 2: bfloat16 [256, 1536], P(('dp', 'ep'))
All inputs are finite; a program needn't handle non-finite values.
Results may differ from the reference program's by a relative error of at most 0.0137999.
Values are sent between devices in bfloat16 or wider.
A program may use at most 1 GiB of HBM per device.

```python
import jax
import jax.numpy as jnp
from jax import lax

MODEL_DIM = 1536
FFN_DIM = 512
EXPERTS = 40
TOP_K = 8
HEADS = 24
TOKENS = 32
GROUP = 8
SLOTS = 8

HEAD_DIM = MODEL_DIM // HEADS
ROWS = GROUP * TOKENS
NORM_EPS = 1e-6
MASK_VALUE = -1e30


def draw_routing(route_key):
    key_start, key_hot, key_pick = jax.random.split(route_key, 3)
    spacing = EXPERTS // TOP_K
    hot_span = max(1, EXPERTS // (4 * TOP_K))
    start_any = jax.random.randint(key_start, (ROWS,), 0, EXPERTS)
    start_hot = jax.random.randint(key_hot, (ROWS,), 0, hot_span)
    use_hot = jax.random.randint(key_pick, (ROWS,), 0, 2) == 1
    position = jnp.arange(ROWS) % TOKENS
    first_expert = jnp.where(use_hot, start_hot, start_any)
    first_expert = jnp.where(position <= SLOTS, 0, first_expert)
    choice = (first_expert[:, None] + spacing * jnp.arange(TOP_K)[None, :]) % EXPERTS
    choice = choice.astype(jnp.int32)

    def device_slots(dev_choice):
        flat_ids = dev_choice.reshape(-1)
        onehot = (flat_ids[:, None] == jnp.arange(EXPERTS)[None, :]).astype(jnp.int32)
        rank_pos = jnp.sum(jnp.cumsum(onehot, axis=0) * onehot, axis=1) - 1
        return jnp.where(rank_pos < SLOTS, rank_pos, -1).reshape(TOKENS, TOP_K)

    slot_ids = lax.map(device_slots, choice.reshape(GROUP, TOKENS, TOP_K))
    return choice, slot_ids.reshape(ROWS, TOP_K).astype(jnp.int32)


def setup_inputs(seed: int = 0, part: int = 0) -> dict:
    base_key = jax.random.key(seed)
    part_key = jax.random.fold_in(base_key, part)
    part_keys = jax.random.split(part_key, 6)
    shared_keys = jax.random.split(base_key, 9)
    scale_in = MODEL_DIM ** -0.5
    scale_ffn = FFN_DIM ** -0.5
    experts_a, slots_a = draw_routing(part_keys[1])
    experts_b, slots_b = draw_routing(part_keys[4])
    return {
        "tokens_a": jax.random.normal(part_keys[0], (ROWS, MODEL_DIM), jnp.float32).astype(jnp.bfloat16),
        "experts_a": experts_a,
        "slots_a": slots_a,
        "gates_a": jax.random.uniform(part_keys[2], (ROWS, TOP_K), jnp.float32, 0.5, 1.5).astype(jnp.bfloat16),
        "tokens_b": jax.random.normal(part_keys[3], (ROWS, MODEL_DIM), jnp.float32).astype(jnp.bfloat16),
        "experts_b": experts_b,
        "slots_b": slots_b,
        "gates_b": jax.random.uniform(part_keys[5], (ROWS, TOP_K), jnp.float32, 0.5, 1.5).astype(jnp.bfloat16),
        "attn_gain": (1.0 + 0.3 * jax.random.normal(shared_keys[0], (MODEL_DIM,), jnp.float32)).astype(jnp.bfloat16),
        "w_query": (1.5 * scale_in * jax.random.normal(shared_keys[1], (MODEL_DIM, HEADS, HEAD_DIM), jnp.float32)).astype(jnp.bfloat16),
        "w_key": (1.5 * scale_in * jax.random.normal(shared_keys[2], (MODEL_DIM, HEADS, HEAD_DIM), jnp.float32)).astype(jnp.bfloat16),
        "w_value": (scale_in * jax.random.normal(shared_keys[3], (MODEL_DIM, HEADS, HEAD_DIM), jnp.float32)).astype(jnp.bfloat16),
        "w_out": (scale_in * jax.random.normal(shared_keys[4], (HEADS, HEAD_DIM, MODEL_DIM), jnp.float32)).astype(jnp.bfloat16),
        "moe_gain": (1.0 + 0.3 * jax.random.normal(shared_keys[5], (MODEL_DIM,), jnp.float32)).astype(jnp.bfloat16),
        "w_gate": (scale_in * jax.random.normal(shared_keys[6], (EXPERTS, MODEL_DIM, FFN_DIM), jnp.float32)).astype(jnp.bfloat16),
        "w_up": (scale_in * jax.random.normal(shared_keys[7], (EXPERTS, MODEL_DIM, FFN_DIM), jnp.float32)).astype(jnp.bfloat16),
        "w_down": (scale_ffn * jax.random.normal(shared_keys[8], (EXPERTS, FFN_DIM, MODEL_DIM), jnp.float32)).astype(jnp.bfloat16),
    }


def rms_norm(rows, gain_vec):
    rows_f = rows.astype(jnp.float32)
    inv_rms = lax.rsqrt(jnp.mean(rows_f * rows_f, axis=-1, keepdims=True) + NORM_EPS)
    return (rows_f * inv_rms * gain_vec.astype(jnp.float32)).astype(jnp.bfloat16)


def attention_block(sequence, attn_gain, w_query, w_key, w_value, w_out):
    normed = rms_norm(sequence, attn_gain).astype(jnp.float32)
    query = jnp.einsum("td,dhe->the", normed, w_query.astype(jnp.float32)).astype(jnp.bfloat16)
    keys = jnp.einsum("td,dhe->the", normed, w_key.astype(jnp.float32)).astype(jnp.bfloat16)
    values = jnp.einsum("td,dhe->the", normed, w_value.astype(jnp.float32)).astype(jnp.bfloat16)
    scores = jnp.einsum("qhe,khe->hqk", query.astype(jnp.float32), keys.astype(jnp.float32)) * (HEAD_DIM ** -0.5)
    causal = jnp.arange(TOKENS)[:, None] >= jnp.arange(TOKENS)[None, :]
    scores = jnp.where(causal[None, :, :], scores, MASK_VALUE)
    attn_prob = jax.nn.softmax(scores, axis=-1).astype(jnp.bfloat16)
    context = jnp.einsum("hqk,khe->qhe", attn_prob.astype(jnp.float32), values.astype(jnp.float32)).astype(jnp.bfloat16)
    attn_out = jnp.einsum("qhe,hed->qd", context.astype(jnp.float32), w_out.astype(jnp.float32))
    return (sequence.astype(jnp.float32) + attn_out).astype(jnp.bfloat16)


def moe_layer(tokens, experts, slots, gates, attn_gain, w_query, w_key, w_value, w_out, moe_gain, w_gate, w_up, w_down):
    residual = lax.map(lambda sequence: attention_block(sequence, attn_gain, w_query, w_key, w_value, w_out), tokens.reshape(GROUP, TOKENS, MODEL_DIM))
    normed = rms_norm(residual, moe_gain).reshape(ROWS, MODEL_DIM)
    row_ids = jnp.arange(ROWS, dtype=jnp.int32)
    owner = row_ids // TOKENS
    buffer_rows = EXPERTS * GROUP * SLOTS
    dest_row = jnp.where(slots >= 0, experts * (GROUP * SLOTS) + owner[:, None] * SLOTS + slots, buffer_rows)
    token_of = jnp.broadcast_to(row_ids[:, None], (ROWS, TOP_K)).reshape(-1)
    source = jnp.full((buffer_rows,), ROWS, jnp.int32).at[dest_row.reshape(-1)].set(token_of, mode="drop")

    def expert_ffn(operands):
        expert_source, gate_w, up_w, down_w = operands
        rows_in = jnp.take(normed, expert_source, axis=0, mode="fill", fill_value=0)
        gate_act = jnp.dot(rows_in, gate_w, preferred_element_type=jnp.float32)
        up_act = jnp.dot(rows_in, up_w, preferred_element_type=jnp.float32)
        hidden = (jax.nn.silu(gate_act) * up_act).astype(jnp.bfloat16)
        return jnp.dot(hidden, down_w, preferred_element_type=jnp.float32).astype(jnp.bfloat16)

    expert_out = lax.map(expert_ffn, (source.reshape(EXPERTS, GROUP * SLOTS), w_gate, w_up, w_down)).reshape(buffer_rows, MODEL_DIM)

    def combine(operands):
        dev_resid, dev_dest, dev_gates = operands
        picked = jnp.take(expert_out, dev_dest, axis=0, mode="fill", fill_value=0).reshape(TOKENS, TOP_K, MODEL_DIM)
        mixed_sum = jnp.einsum("tk,tkd->td", dev_gates.astype(jnp.float32), picked.astype(jnp.float32))
        return (dev_resid.astype(jnp.float32) + mixed_sum).astype(jnp.bfloat16)

    mixed_rows = lax.map(combine, (residual, dest_row.reshape(GROUP, TOKENS * TOP_K), gates.reshape(GROUP, TOKENS, TOP_K)))
    return mixed_rows.reshape(ROWS, MODEL_DIM)


def reference(tokens_a, experts_a, slots_a, gates_a, tokens_b, experts_b, slots_b, gates_b, attn_gain, w_query, w_key, w_value, w_out, moe_gain, w_gate, w_up, w_down):
    out_a = moe_layer(tokens_a, experts_a, slots_a, gates_a, attn_gain, w_query, w_key, w_value, w_out, moe_gain, w_gate, w_up, w_down)
    out_b = moe_layer(tokens_b, experts_b, slots_b, gates_b, attn_gain, w_query, w_key, w_value, w_out, moe_gain, w_gate, w_up, w_down)
    return (out_a, out_b)
```

```python
import functools

import jax
import jax.numpy as jnp
from jax import lax
from jax.experimental import pallas as pl
from jax.experimental.pallas import tpu as pltpu
from jax.sharding import PartitionSpec as P

NORM_EPS = 1e-6
MASK_VALUE = -1e30
MESH = pl.DeviceIdType.MESH

GROUP = 8
TOKENS = 32
DIM = 1536
FFN = 512
LOCAL = 5
SLOTS = 8
HALF = DIM // 2
CHUNK = 256
CHUNKS = DIM // CHUNK
ROWS = GROUP * TOKENS
LROWS = LOCAL * GROUP * SLOTS
F32 = jnp.float32
BF16 = jnp.bfloat16

NT = (((1,), (1,)), ((), ()))
TN = (((0,), (0,)), ((), ()))


def rms_rows(rows_f, gain):
    inv = lax.rsqrt(jnp.mean(rows_f * rows_f, axis=-1, keepdims=True) + NORM_EPS)
    return (rows_f * inv * gain).astype(BF16)


def kernel(
    tok_a, exp_a, slot_a, gate_a, tok_b, exp_b, slot_b, gate_b,
    again_hbm, wq_hbm, wk_hbm, wv_hbm, wo_hbm, mgain_hbm, wg_hbm, wu_hbm, wd_hbm,
    out_a, out_b,
    xv, gains, ev, sv, gv,
    wqkv, wov, wgv, wuv, wdv,
    norm_a, qkv, ctx, hv, uall, meta, disp, comb, picked, o2, part, r1, s2, r2, fin, r3, yv,
    sem_in, sem_qkv, sem_o, sem_exp, sem_out,
    msend, mrecv, dsend, drecv, osend, orecv, rsend, rrecv,
):
    me = lax.axis_index("ep")
    core = me % 2
    px = (me // 2) % 2
    py = me // 4
    flip1 = me + 1 - 2 * core
    flip2 = me + 2 - 4 * px
    flip4 = me + 4 - 8 * py
    flip = {
        1: flip1,
        2: flip2,
        4: flip4,
        3: flip2 + 1 - 2 * core,
        5: flip4 + 1 - 2 * core,
        6: flip2 + 4 - 8 * py,
    }
    flip[7] = flip[6] + 1 - 2 * core
    first = (1 - core) * flip2 + core * flip4
    second = (1 - core) * flip4 + core * flip2

    def local(src, dst, sem):
        return pltpu.make_async_copy(src, dst, sem)

    def remote(src, dst, ssem, rsem, dev):
        return pltpu.make_async_remote_copy(
            src_ref=src, dst_ref=dst, send_sem=ssem, recv_sem=rsem,
            device_id={"ep": dev}, device_id_type=MESH,
        )

    small = [
        local(exp_a, ev.at[0], sem_in.at[0]),
        local(exp_b, ev.at[1], sem_in.at[1]),
        local(slot_a, sv.at[0], sem_in.at[2]),
        local(slot_b, sv.at[1], sem_in.at[3]),
        local(gate_a, gv.at[0], sem_in.at[4]),
        local(gate_b, gv.at[1], sem_in.at[5]),
        local(tok_a, xv.at[pl.ds(0, TOKENS)], sem_in.at[6]),
        local(tok_b, xv.at[pl.ds(TOKENS, TOKENS)], sem_in.at[7]),
        local(again_hbm, gains.at[0], sem_in.at[8]),
        local(mgain_hbm, gains.at[1], sem_in.at[9]),
    ]
    for copy in small:
        copy.start()

    whbm = (wq_hbm, wk_hbm, wv_hbm)

    def qkv_copy(which, c):
        rows = pl.ds(pl.multiple_of(c * CHUNK, CHUNK), CHUNK)
        return local(whbm[which].at[rows], wqkv.at[which, c], sem_qkv.at[which, c])

    for c in range(CHUNKS):
        for which in range(3):
            qkv_copy(which, c).start()
    wo_copy = local(wo_hbm, wov, sem_o)
    wo_copy.start()

    barrier = pltpu.get_barrier_semaphore()
    for k in range(1, GROUP):
        pl.semaphore_signal(barrier, inc=1, device_id={"ep": flip[k]}, device_id_type=MESH)

    for copy in small[:6]:
        copy.wait()

    lane = lax.broadcasted_iota(jnp.int32, (SLOTS, 128), 1)
    my_lanes = lane // TOKENS == me % 4
    for b in range(2):
        code = jnp.where(sv[b] >= 0, ev[b] * SLOTS + sv[b], -1).astype(F32)
        code = jnp.concatenate([code] * 4, axis=1)
        gate = jnp.concatenate([gv[b].astype(F32)] * 4, axis=1)
        meta[me, b, 0] = jnp.where(my_lanes, code, -1.0)
        meta[me, b, 1] = jnp.where(my_lanes, gate, 0.0)

    pl.semaphore_wait(barrier, GROUP - 1)

    def meta_copy(k):
        return remote(meta.at[me], meta.at[me], msend.at[k], mrecv.at[k], flip[k])

    for k in range(1, GROUP):
        meta_copy(k).start()

    for copy in small[6:]:
        copy.wait()
    norm_a[...] = rms_rows(xv[...].astype(F32), gains[0].astype(F32))

    def qkv_step(c, carry):
        for which in range(3):
            qkv_copy(which, c).wait()
        for which in range(3):
            prod = lax.dot_general(norm_a[...], wqkv[which, c], NT, preferred_element_type=F32)
            qkv[which, c] = prod.astype(BF16)
        return carry

    lax.fori_loop(0, CHUNKS, qkv_step, 0)

    def expert_copies(e):
        return (
            local(wg_hbm.at[e], wgv.at[e], sem_exp.at[0, e]),
            local(wu_hbm.at[e], wuv.at[e], sem_exp.at[1, e]),
            local(wd_hbm.at[e], wdv.at[e], sem_exp.at[2, e]),
        )

    for e in range(LOCAL):
        for copy in expert_copies(e):
            copy.start()

    n2 = 2 * TOKENS
    lane128 = lax.broadcasted_iota(jnp.int32, (n2, 128), 1)
    row128 = lax.broadcasted_iota(jnp.int32, (n2, 128), 0)
    key = lane128 % n2
    visible = (key // TOKENS == row128 // TOKENS) & (key <= row128)
    low = lane128 < n2
    scale = 64.0 ** -0.5
    for pair in range(DIM // 128):
        c, off = pair // 2, (pair % 2) * 128
        q = qkv[0, c, :, off:off + 128]
        k = qkv[1, c, :, off:off + 128]
        v = qkv[2, c, :, off:off + 128]
        zero = jnp.zeros_like(k)
        kk = jnp.concatenate([jnp.where(low, k, zero), jnp.where(low, zero, k)], axis=0)
        vv = jnp.concatenate([jnp.where(low, v, zero), jnp.where(low, zero, v)], axis=0)
        s = lax.dot_general(q, kk, NT, preferred_element_type=F32) * scale
        s = jnp.where(visible, s, MASK_VALUE)
        m0 = jnp.max(jnp.where(low, s, -jnp.inf), axis=-1, keepdims=True)
        m1 = jnp.max(jnp.where(low, -jnp.inf, s), axis=-1, keepdims=True)
        p = jnp.exp(s - jnp.where(low, m0, m1))
        d0 = jnp.sum(jnp.where(low, p, 0.0), axis=-1, keepdims=True)
        d1 = jnp.sum(jnp.where(low, 0.0, p), axis=-1, keepdims=True)
        p = (p / jnp.where(low, d0, d1)).astype(BF16)
        ctx[:, pair * 128:(pair + 1) * 128] = jnp.dot(p, vv, preferred_element_type=F32).astype(BF16)

    wo_copy.wait()
    attn = jnp.dot(ctx[...], wov[...], preferred_element_type=F32)
    h = (xv[...].astype(F32) + attn).astype(BF16)
    hv[...] = h
    u = rms_rows(h.astype(F32), gains[1].astype(F32))
    my_rows = pl.ds(pl.multiple_of(me * TOKENS, TOKENS), TOKENS)
    uall[0, my_rows, :] = u[:TOKENS]
    uall[1, my_rows, :] = u[TOKENS:]

    def block(b, dev, lo=0, n=TOKENS):
        return uall.at[b, pl.ds(pl.multiple_of(dev * TOKENS + lo, 16), n)]

    def disp_copy(b, i, dev_block, target, slot, lo=0, n=TOKENS):
        ref = block(b, dev_block, lo, n)
        return remote(ref, ref, dsend.at[b, i], drecv.at[b, slot], target)

    H = TOKENS // 2

    def d_near_x(b):
        return disp_copy(b, 0, me, flip[2], 2)

    def d_near_y(b):
        return disp_copy(b, 1, me, flip[4], 4)

    def d_sib(b):
        return disp_copy(b, 2, me, flip[1], 1)

    def d_fwd_x(b):
        return disp_copy(b, 3, flip[2], flip[4], 6, 0, H)

    def d_fwd_y(b):
        return disp_copy(b, 4, flip[4], flip[2], 0, H, H)

    def d_sib_x(b):
        return disp_copy(b, 5, flip[2], flip[1], 3)

    def d_sib_y(b):
        return disp_copy(b, 6, flip[4], flip[1], 5)

    def d_sib_d(b):
        return disp_copy(b, 7, flip[6], flip[1], 7)

    def d_wait(b, slot, dev, lo=0, n=TOKENS):
        ref = block(b, dev, lo, n)
        remote(ref, ref, dsend.at[b, 0], drecv.at[b, slot], flip[1]).wait_recv()

    for b in range(2):
        d_near_x(b).start()
        d_near_y(b).start()
        d_sib(b).start()

    for k in range(1, GROUP):
        remote(meta.at[flip[k]], meta.at[flip[k]], msend.at[k], mrecv.at[k], flip[k]).wait_recv()

    slot_row = lax.broadcasted_iota(jnp.int32, (SLOTS, ROWS), 0)
    row64 = lax.broadcasted_iota(jnp.int32, (GROUP * SLOTS, ROWS), 0)
    lane64 = lax.broadcasted_iota(jnp.int32, (GROUP * SLOTS, ROWS), 1)
    owner_hit = lane64 // TOKENS == row64 // SLOTS
    for b in range(2):
        halves = []
        for kind in range(2):
            parts = []
            for side in range(2):
                acc = meta[4 * side, b, kind]
                for p in range(1, 4):
                    acc = jnp.maximum(acc, meta[4 * side + p, b, kind])
                parts.append(acc)
            halves.append(jnp.concatenate(parts, axis=1))
        code, gate = halves
        code_rows = [jnp.broadcast_to(code[j:j + 1], (SLOTS, ROWS)) for j in range(SLOTS)]
        gate_rows = [jnp.broadcast_to(gate[j:j + 1], (SLOTS, ROWS)) for j in range(SLOTS)]
        for who in range(2):
            dev = me if who == 0 else flip[1]
            for e in range(LOCAL):
                target = ((dev * LOCAL + e) * SLOTS + slot_row).astype(F32)
                hit = jnp.zeros((SLOTS, ROWS), F32)
                weight = jnp.zeros((SLOTS, ROWS), F32)
                for j in range(SLOTS):
                    match = code_rows[j] == target
                    weight = weight + jnp.where(match, gate_rows[j], 0.0)
                    if who == 0:
                        hit = hit + jnp.where(match, 1.0, 0.0)
                rows = slice((who * LOCAL + e) * 64, (who * LOCAL + e + 1) * 64)
                wide = jnp.concatenate([weight] * GROUP, axis=0)
                comb[b, rows, :] = jnp.where(owner_hit, wide, 0.0).astype(BF16)
                if who == 0:
                    wide = jnp.concatenate([hit] * GROUP, axis=0)
                    disp[b, e * 64:(e + 1) * 64, :] = jnp.where(owner_hit, wide, 0.0).astype(BF16)

    def relay(b):
        d_wait(b, 2, flip[2])
        d_fwd_x(b).start()
        d_sib_x(b).start()
        d_wait(b, 4, flip[4])
        d_fwd_y(b).start()
        d_sib_y(b).start()

    def relay_far(b):
        d_wait(b, 6, flip[6], 0, H)
        d_wait(b, 0, flip[6], H, H)
        d_sib_d(b).start()

    def gathered(b):
        d_wait(b, 1, flip[1])
        d_wait(b, 3, flip[3])
        d_wait(b, 5, flip[5])
        d_wait(b, 7, flip[7])

    def pick(b):
        def pick_step(n, carry):
            cols = pl.ds(pl.multiple_of(n * CHUNK, CHUNK), CHUNK)
            picked[:, cols] = jnp.dot(disp[b], uall[b, :, cols], preferred_element_type=F32).astype(BF16)
            return carry

        lax.fori_loop(0, CHUNKS, pick_step, 0)

    def experts(b):
        def expert_step(e, carry):
            if b == 0:
                for copy in expert_copies(e):
                    copy.wait()
            rows = pl.ds(pl.multiple_of(e * 64, 64), 64)
            x = picked[rows, :]
            g = jnp.dot(x, wgv[e], preferred_element_type=F32)
            up = jnp.dot(x, wuv[e], preferred_element_type=F32)
            hidden = (g * (1.0 / (1.0 + jnp.exp(-g))) * up).astype(BF16)
            o = jnp.dot(hidden, wdv[e], preferred_element_type=F32).astype(BF16)
            o2[b, 0, rows, :] = o[:, :HALF]
            o2[b, 1, rows, :] = o[:, HALF:]
            return carry

        lax.fori_loop(0, LOCAL, expert_step, 0)

    def o_copy(b):
        src = o2.at[b, 1 - core, pl.ds(0, LROWS)]
        dst = o2.at[b, 1 - core, pl.ds(LROWS, LROWS)]
        return remote(src, dst, osend.at[b], orecv.at[b], flip[1])

    def o_wait(b):
        ref = o2.at[b, core, pl.ds(LROWS, LROWS)]
        remote(ref, ref, osend.at[b], orecv.at[b], flip[1]).wait_recv()

    def combine(b):
        for n in range(HALF // CHUNK):
            cols = slice(n * CHUNK, (n + 1) * CHUNK)
            part[b, :, cols] = lax.dot_general(comb[b], o2[b, core, :, cols], TN, preferred_element_type=F32)

    def chip_rows(ref, b, dev):
        return ref.at[b, pl.ds(pl.multiple_of((dev // 2) * 64, 64), 64)]

    def far_copy(b):
        return remote(chip_rows(part, b, flip[6]), r1.at[b, 1], rsend.at[b, 0], rrecv.at[b, 0], first)

    def near_copy(b):
        return remote(chip_rows(part, b, first), r1.at[b, 0], rsend.at[b, 1], rrecv.at[b, 1], first)

    def second_copy(b):
        return remote(s2.at[b], r2.at[b], rsend.at[b, 2], rrecv.at[b, 2], second)

    def last_copy(b):
        rows = pl.ds(pl.multiple_of((1 - core) * TOKENS, TOKENS), TOKENS)
        return remote(fin.at[b, rows], r3.at[b], rsend.at[b, 3], rrecv.at[b, 3], flip[1])

    def wide_rows(dev):
        return pl.ds(pl.multiple_of((dev // 2) * 64, 64), 64)

    def fold(b):
        far_copy(b).wait_recv()
        s2[b] = part[b, wide_rows(second), :] + r1[b, 1]
        second_copy(b).start()

    def finish(b):
        near_copy(b).wait_recv()
        second_copy(b).wait_recv()
        fin[b] = part[b, wide_rows(me), :] + r1[b, 0] + r2[b]
        last_copy(b).start()

    def write_out(b, out):
        last_copy(b).wait_recv()
        mine = fin[b, pl.ds(pl.multiple_of(core * TOKENS, TOKENS), TOKENS), :]
        other = r3[b]
        left = jnp.where(core == 0, mine, other)
        right = jnp.where(core == 0, other, mine)
        rows = slice(b * TOKENS, (b + 1) * TOKENS)
        yv[b, :, :HALF] = (hv[rows, :HALF].astype(F32) + left).astype(BF16)
        yv[b, :, HALF:] = (hv[rows, HALF:].astype(F32) + right).astype(BF16)
        copy = local(yv.at[b], out, sem_out.at[b])
        copy.start()
        return copy

    relay(0)
    relay_far(0)
    gathered(0)
    pick(0)
    relay(1)
    experts(0)
    o_copy(0).start()
    relay_far(1)
    o_wait(0)
    combine(0)
    far_copy(0).start()
    near_copy(0).start()
    gathered(1)
    pick(1)
    experts(1)
    o_copy(1).start()
    fold(0)
    o_wait(1)
    combine(1)
    far_copy(1).start()
    near_copy(1).start()
    finish(0)
    fold(1)
    done_a = write_out(0, out_a)
    finish(1)
    done_b = write_out(1, out_b)

    for k in range(1, GROUP):
        meta_copy(k).wait_send()
    for b in range(2):
        for make in (d_near_x, d_near_y, d_sib, d_fwd_x, d_fwd_y, d_sib_x, d_sib_y, d_sib_d, o_copy, far_copy, near_copy, second_copy, last_copy):
            make(b).wait_send()
    done_a.wait()
    done_b.wait()


def solution(mesh):
    row_spec = P(("dp", "ep"), None)
    full_spec = P(None, None, None)
    gain_spec = P(None)
    expert_spec = P("ep", None, None)
    in_specs = (row_spec,) * 8 + (gain_spec,) + (full_spec,) * 4 + (gain_spec,) + (expert_spec,) * 3

    any_spec = pl.BlockSpec(memory_space=pl.ANY)
    VM = pltpu.VMEM
    DMA = pltpu.SemaphoreType.DMA
    scratch = [
        VM((2 * TOKENS, DIM), BF16),
        VM((2, 1, DIM), BF16),
        VM((2, SLOTS, TOKENS), jnp.int32),
        VM((2, SLOTS, TOKENS), jnp.int32),
        VM((2, SLOTS, TOKENS), BF16),
        VM((3, CHUNKS, CHUNK, DIM), BF16),
        VM((DIM, DIM), BF16),
        VM((LOCAL, DIM, FFN), BF16),
        VM((LOCAL, DIM, FFN), BF16),
        VM((LOCAL, FFN, DIM), BF16),
        VM((2 * TOKENS, DIM), BF16),
        VM((3, CHUNKS, 2 * TOKENS, CHUNK), BF16),
        VM((2 * TOKENS, DIM), BF16),
        VM((2 * TOKENS, DIM), BF16),
        VM((2, ROWS, DIM), BF16),
        VM((GROUP, 2, 2, SLOTS, 128), F32),
        VM((2, LROWS, ROWS), BF16),
        VM((2, 2 * LROWS, ROWS), BF16),
        VM((LROWS, DIM), BF16),
        VM((2, 2, 2 * LROWS, HALF), BF16),
        VM((2, ROWS, HALF), F32),
        VM((2, 2, 2 * TOKENS, HALF), F32),
        VM((2, 2 * TOKENS, HALF), F32),
        VM((2, 2 * TOKENS, HALF), F32),
        VM((2, 2 * TOKENS, HALF), F32),
        VM((2, TOKENS, HALF), F32),
        VM((2, TOKENS, DIM), BF16),
        DMA((10,)),
        DMA((3, CHUNKS)),
        DMA,
        DMA((3, LOCAL)),
        DMA((2,)),
        DMA((GROUP,)),
        DMA((GROUP,)),
        DMA((2, 8)),
        DMA((2, 8)),
        DMA((2,)),
        DMA((2,)),
        DMA((2, 4)),
        DMA((2, 4)),
    ]

    def device_fn(tokens_a, experts_a, slots_a, gates_a, tokens_b, experts_b, slots_b, gates_b, attn_gain, w_query, w_key, w_value, w_out, moe_gain, w_gate, w_up, w_down):
        def heads_first(w):
            return jnp.transpose(w, (1, 2, 0)).reshape(DIM, DIM)

        out = jax.ShapeDtypeStruct((TOKENS, DIM), BF16)
        return pl.pallas_call(
            kernel,
            out_shape=(out, out),
            in_specs=[any_spec] * 17,
            out_specs=(any_spec, any_spec),
            scratch_shapes=scratch,
            compiler_params=pltpu.CompilerParams(
                collective_id=0, has_side_effects=True, vmem_limit_bytes=66_000_000,
            ),
            name="moe_layer",
        )(
            tokens_a, experts_a.T, slots_a.T, gates_a.T, tokens_b, experts_b.T, slots_b.T, gates_b.T,
            attn_gain.reshape(1, DIM), heads_first(w_query), heads_first(w_key), heads_first(w_value),
            w_out.reshape(DIM, DIM), moe_gain.reshape(1, DIM), w_gate, w_up, w_down,
        )

    return jax.shard_map(device_fn, mesh=mesh, in_specs=in_specs, out_specs=(row_spec, row_spec), check_vma=False)
```

```python
import functools

import jax
import jax.numpy as jnp
from jax import lax
from jax.experimental import pallas as pl
from jax.experimental.pallas import tpu as pltpu
from jax.sharding import PartitionSpec as P

NORM_EPS = 1e-6
MASK_VALUE = -1e30
MESH = pl.DeviceIdType.MESH

GROUP = 8
TOKENS = 32
DIM = 1536
FFN = 512
LOCAL = 5
SLOTS = 8
HALF = DIM // 2
CHUNK = 256
CHUNKS = DIM // CHUNK
ROWS = GROUP * TOKENS
LROWS = LOCAL * GROUP * SLOTS
F32 = jnp.float32
BF16 = jnp.bfloat16

NT = (((1,), (1,)), ((), ()))
TN = (((0,), (0,)), ((), ()))


def rms_rows(rows_f, gain):
    inv = lax.rsqrt(jnp.mean(rows_f * rows_f, axis=-1, keepdims=True) + NORM_EPS)
    return (rows_f * inv * gain).astype(BF16)


def kernel(
    tok_a, exp_a, slot_a, gate_a, tok_b, exp_b, slot_b, gate_b,
    again_hbm, wq_hbm, wk_hbm, wv_hbm, wo_hbm, mgain_hbm, wg_hbm, wu_hbm, wd_hbm,
    out_a, out_b,
    xv, gains, ev, sv, gv,
    wqkv, wov, wgv, wuv, wdv,
    norm_a, qkv, ctx, hv, uall, meta, disp, comb, picked, o2, part, r1, s2, r2, fin, r3, yv,
    sem_in, sem_qkv, sem_o, sem_exp, sem_out,
    msend, mrecv, dsend, drecv, osend, orecv, rsend, rrecv,
):
    me = lax.axis_index("ep")
    core = me % 2
    px = (me // 2) % 2
    py = me // 4
    flip1 = me + 1 - 2 * core
    flip2 = me + 2 - 4 * px
    flip4 = me + 4 - 8 * py
    flip = {
        1: flip1,
        2: flip2,
        4: flip4,
        3: flip2 + 1 - 2 * core,
        5: flip4 + 1 - 2 * core,
        6: flip2 + 4 - 8 * py,
    }
    flip[7] = flip[6] + 1 - 2 * core
    first = (1 - core) * flip2 + core * flip4
    second = (1 - core) * flip4 + core * flip2

    def local(src, dst, sem):
        return pltpu.make_async_copy(src, dst, sem)

    def remote(src, dst, ssem, rsem, dev):
        return pltpu.make_async_remote_copy(
            src_ref=src, dst_ref=dst, send_sem=ssem, recv_sem=rsem,
            device_id={"ep": dev}, device_id_type=MESH,
        )

    small = [
        local(exp_a, ev.at[0], sem_in.at[0]),
        local(exp_b, ev.at[1], sem_in.at[1]),
        local(slot_a, sv.at[0], sem_in.at[2]),
        local(slot_b, sv.at[1], sem_in.at[3]),
        local(gate_a, gv.at[0], sem_in.at[4]),
        local(gate_b, gv.at[1], sem_in.at[5]),
        local(tok_a, xv.at[pl.ds(0, TOKENS)], sem_in.at[6]),
        local(tok_b, xv.at[pl.ds(TOKENS, TOKENS)], sem_in.at[7]),
        local(again_hbm, gains.at[0], sem_in.at[8]),
        local(mgain_hbm, gains.at[1], sem_in.at[9]),
    ]
    for copy in small:
        copy.start()

    whbm = (wq_hbm, wk_hbm, wv_hbm)

    def qkv_copy(which, c):
        rows = pl.ds(pl.multiple_of(c * CHUNK, CHUNK), CHUNK)
        return local(whbm[which].at[rows], wqkv.at[which, c], sem_qkv.at[which, c])

    for which in range(3):
        qkv_copy(which, 0).start()
    wo_copy = local(wo_hbm, wov, sem_o)

    barrier = pltpu.get_barrier_semaphore()
    for k in range(1, GROUP):
        pl.semaphore_signal(barrier, inc=1, device_id={"ep": flip[k]}, device_id_type=MESH)

    for copy in small:
        copy.wait()
    for c in range(1, CHUNKS):
        for which in range(3):
            qkv_copy(which, c).start()
    wo_copy.start()

    def gain_row(i):
        g = gains[i].astype(F32)
        return jnp.concatenate([g[j:j + 1] for j in range(DIM // 128)], axis=1)

    norm_a[...] = rms_rows(xv[...].astype(F32), gain_row(0))

    lane = lax.broadcasted_iota(jnp.int32, (SLOTS, 128), 1)
    my_lanes = lane // TOKENS == me % 4
    for b in range(2):
        code = jnp.where(sv[b] >= 0, ev[b] * SLOTS + sv[b], -1).astype(F32)
        code = jnp.concatenate([code] * 4, axis=1)
        gate = jnp.concatenate([gv[b].astype(F32)] * 4, axis=1)
        meta[me, b, 0] = jnp.where(my_lanes, code, -1.0)
        meta[me, b, 1] = jnp.where(my_lanes, gate, 0.0)

    pl.semaphore_wait(barrier, GROUP - 1)

    def meta_copy(k):
        return remote(meta.at[me], meta.at[me], msend.at[k], mrecv.at[k], flip[k])

    for k in range(1, GROUP):
        meta_copy(k).start()


    n2 = 2 * TOKENS
    lane128 = lax.broadcasted_iota(jnp.int32, (n2, 128), 1)
    row128 = lax.broadcasted_iota(jnp.int32, (n2, 128), 0)
    key = lane128 % n2
    visible = (key // TOKENS == row128 // TOKENS) & (key <= row128)
    low = lane128 < n2
    head_of = lax.broadcasted_iota(jnp.int32, (n2, CHUNK), 1) // n2
    scale = 64.0 ** -0.5

    def spread(x):
        zero = jnp.zeros_like(x)
        return jnp.concatenate([jnp.where(head_of == g, x, zero) for g in range(CHUNK // n2)], axis=0)

    def softmax_pair(s):
        s = jnp.where(visible, s * scale, MASK_VALUE)
        m0 = jnp.max(jnp.where(low, s, -jnp.inf), axis=-1, keepdims=True)
        m1 = jnp.max(jnp.where(low, -jnp.inf, s), axis=-1, keepdims=True)
        p = jnp.exp(s - jnp.where(low, m0, m1))
        d0 = jnp.sum(jnp.where(low, p, 0.0), axis=-1, keepdims=True)
        d1 = jnp.sum(jnp.where(low, 0.0, p), axis=-1, keepdims=True)
        return (p / jnp.where(low, d0, d1)).astype(BF16)

    def project(which, c):
        prod = lax.dot_general(norm_a[...], wqkv[which, c], NT, preferred_element_type=F32)
        return prod.astype(BF16)

    def scores(c):
        return lax.dot_general(qkv[0, c], spread(qkv[1, c]), NT, preferred_element_type=F32)

    def softmax(s):
        return jnp.concatenate([softmax_pair(s[:, i * 128:(i + 1) * 128]) for i in range(CHUNK // 128)], axis=1)

    def store_context(c, p, values):
        ctx[:, pl.ds(pl.multiple_of(c * CHUNK, CHUNK), CHUNK)] = jnp.dot(p, values, preferred_element_type=F32).astype(BF16)

    def wait_chunk(c):
        for which in range(3):
            qkv_copy(which, c).wait()

    wait_chunk(0)
    for which in range(3):
        qkv[which, 0] = project(which, 0)

    def qkv_step(c, carry):
        wait_chunk(c)
        values = spread(qkv[2, c - 1])
        s = scores(c - 1)
        q = project(0, c)
        p = softmax(s)
        k = project(1, c)
        store_context(c - 1, p, values)
        v = project(2, c)
        qkv[0, c] = q
        qkv[1, c] = k
        qkv[2, c] = v
        return carry

    lax.fori_loop(1, CHUNKS, qkv_step, 0)

    def expert_copies(e):
        return (
            local(wg_hbm.at[e], wgv.at[e], sem_exp.at[0, e]),
            local(wu_hbm.at[e], wuv.at[e], sem_exp.at[1, e]),
            local(wd_hbm.at[e], wdv.at[e], sem_exp.at[2, e]),
        )

    for e in range(LOCAL):
        for copy in expert_copies(e):
            copy.start()

    store_context(CHUNKS - 1, softmax(scores(CHUNKS - 1)), spread(qkv[2, CHUNKS - 1]))

    wo_copy.wait()
    attn = jnp.dot(ctx[...], wov[...], preferred_element_type=F32)
    h = (xv[...].astype(F32) + attn).astype(BF16)
    hv[...] = h
    u = rms_rows(h.astype(F32), gain_row(1))
    my_rows = pl.ds(pl.multiple_of(me * TOKENS, TOKENS), TOKENS)
    uall[0, my_rows, :] = u[:TOKENS]
    uall[1, my_rows, :] = u[TOKENS:]

    def block(b, dev, lo=0, n=TOKENS):
        return uall.at[b, pl.ds(pl.multiple_of(dev * TOKENS + lo, 16), n)]

    def disp_copy(b, i, dev_block, target, slot, lo=0, n=TOKENS):
        ref = block(b, dev_block, lo, n)
        return remote(ref, ref, dsend.at[b, i], drecv.at[b, slot], target)

    H = TOKENS // 2

    def d_near_x(b):
        return disp_copy(b, 0, me, flip[2], 2)

    def d_near_y(b):
        return disp_copy(b, 1, me, flip[4], 4)

    def d_sib(b):
        return disp_copy(b, 2, me, flip[1], 1)

    def d_fwd_x(b):
        return disp_copy(b, 3, flip[2], flip[4], 6, 0, H)

    def d_fwd_y(b):
        return disp_copy(b, 4, flip[4], flip[2], 0, H, H)

    def d_sib_x(b):
        return disp_copy(b, 5, flip[2], flip[1], 3)

    def d_sib_y(b):
        return disp_copy(b, 6, flip[4], flip[1], 5)

    def d_sib_d(b):
        return disp_copy(b, 7, flip[6], flip[1], 7)

    def d_wait(b, slot, dev, lo=0, n=TOKENS):
        ref = block(b, dev, lo, n)
        remote(ref, ref, dsend.at[b, 0], drecv.at[b, slot], flip[1]).wait_recv()

    for b in range(2):
        d_near_x(b).start()
        d_near_y(b).start()
        d_sib(b).start()

    for k in range(1, GROUP):
        remote(meta.at[flip[k]], meta.at[flip[k]], msend.at[k], mrecv.at[k], flip[k]).wait_recv()

    slot_row = lax.broadcasted_iota(jnp.int32, (SLOTS, ROWS), 0)
    row64 = lax.broadcasted_iota(jnp.int32, (GROUP * SLOTS, ROWS), 0)
    lane64 = lax.broadcasted_iota(jnp.int32, (GROUP * SLOTS, ROWS), 1)
    owner_hit = lane64 // TOKENS == row64 // SLOTS
    for b in range(2):
        halves = []
        for kind in range(2):
            parts = []
            for side in range(2):
                acc = meta[4 * side, b, kind]
                for p in range(1, 4):
                    acc = jnp.maximum(acc, meta[4 * side + p, b, kind])
                parts.append(acc)
            halves.append(jnp.concatenate(parts, axis=1))
        code, gate = halves
        code_rows = [jnp.broadcast_to(code[j:j + 1], (SLOTS, ROWS)) for j in range(SLOTS)]
        gate_rows = [jnp.broadcast_to(gate[j:j + 1], (SLOTS, ROWS)) for j in range(SLOTS)]
        for who in range(2):
            dev = me if who == 0 else flip[1]
            for e in range(LOCAL):
                target = ((dev * LOCAL + e) * SLOTS + slot_row).astype(F32)
                hit = jnp.zeros((SLOTS, ROWS), F32)
                weight = jnp.zeros((SLOTS, ROWS), F32)
                for j in range(SLOTS):
                    match = code_rows[j] == target
                    weight = weight + jnp.where(match, gate_rows[j], 0.0)
                    if who == 0:
                        hit = hit + jnp.where(match, 1.0, 0.0)
                rows = slice((who * LOCAL + e) * 64, (who * LOCAL + e + 1) * 64)
                wide = jnp.concatenate([weight] * GROUP, axis=0)
                comb[b, rows, :] = jnp.where(owner_hit, wide, 0.0).astype(BF16)
                if who == 0:
                    wide = jnp.concatenate([hit] * GROUP, axis=0)
                    disp[b, e * 64:(e + 1) * 64, :] = jnp.where(owner_hit, wide, 0.0).astype(BF16)

    def relay(b):
        d_wait(b, 2, flip[2])
        d_fwd_x(b).start()
        d_sib_x(b).start()
        d_wait(b, 4, flip[4])
        d_fwd_y(b).start()
        d_sib_y(b).start()

    def relay_far(b):
        d_wait(b, 6, flip[6], 0, H)
        d_wait(b, 0, flip[6], H, H)
        d_sib_d(b).start()

    def gathered(b):
        d_wait(b, 1, flip[1])
        d_wait(b, 3, flip[3])
        d_wait(b, 5, flip[5])
        d_wait(b, 7, flip[7])

    def pick(b):
        for n in range(CHUNKS):
            cols = slice(n * CHUNK, (n + 1) * CHUNK)
            picked[:, cols] = jnp.dot(disp[b], uall[b, :, cols], preferred_element_type=F32).astype(BF16)

    def o_copy(b, e):
        src = o2.at[b, 1 - core, pl.ds(e * 64, 64)]
        dst = o2.at[b, 1 - core, pl.ds(LROWS + e * 64, 64)]
        return remote(src, dst, osend.at[b, e], orecv.at[b, e], flip[1])

    def o_wait(b):
        for e in range(LOCAL):
            ref = o2.at[b, core, pl.ds(LROWS + e * 64, 64)]
            remote(ref, ref, osend.at[b, e], orecv.at[b, e], flip[1]).wait_recv()

    def gate_up(e):
        x = picked[e * 64:(e + 1) * 64, :]
        g = jnp.dot(x, wgv[e], preferred_element_type=F32)
        up = jnp.dot(x, wuv[e], preferred_element_type=F32)
        return g, up

    def experts(b):
        if b == 0:
            for e in range(LOCAL):
                for copy in expert_copies(e):
                    copy.wait()
        g, up = gate_up(0)
        for e in range(LOCAL):
            hidden = (g * (1.0 / (1.0 + jnp.exp(-g))) * up).astype(BF16)
            if e + 1 < LOCAL:
                g, up = gate_up(e + 1)
            o = jnp.dot(hidden, wdv[e], preferred_element_type=F32).astype(BF16)
            rows = slice(e * 64, (e + 1) * 64)
            o2[b, 0, rows, :] = o[:, :HALF]
            o2[b, 1, rows, :] = o[:, HALF:]
            if e > 0:
                o_copy(b, e - 1).start()
        o_copy(b, LOCAL - 1).start()

    def combine(b):
        for n in range(HALF // CHUNK):
            cols = slice(n * CHUNK, (n + 1) * CHUNK)
            part[b, :, cols] = lax.dot_general(comb[b], o2[b, core, :, cols], TN, preferred_element_type=F32)

    def chip_rows(ref, b, dev):
        return ref.at[b, pl.ds(pl.multiple_of((dev // 2) * 64, 64), 64)]

    def far_copy(b):
        return remote(chip_rows(part, b, flip[6]), r1.at[b, 1], rsend.at[b, 0], rrecv.at[b, 0], first)

    def near_copy(b):
        return remote(chip_rows(part, b, first), r1.at[b, 0], rsend.at[b, 1], rrecv.at[b, 1], first)

    def second_copy(b):
        return remote(s2.at[b], r2.at[b], rsend.at[b, 2], rrecv.at[b, 2], second)

    def last_copy(b):
        rows = pl.ds(pl.multiple_of((1 - core) * TOKENS, TOKENS), TOKENS)
        return remote(fin.at[b, rows], r3.at[b], rsend.at[b, 3], rrecv.at[b, 3], flip[1])

    def wide_rows(dev):
        return pl.ds(pl.multiple_of((dev // 2) * 64, 64), 64)

    def fold(b):
        far_copy(b).wait_recv()
        s2[b] = part[b, wide_rows(second), :] + r1[b, 1]
        second_copy(b).start()

    def finish(b):
        near_copy(b).wait_recv()
        second_copy(b).wait_recv()
        fin[b] = part[b, wide_rows(me), :] + r1[b, 0] + r2[b]
        last_copy(b).start()

    def write_out(b, out):
        last_copy(b).wait_recv()
        mine = fin[b, pl.ds(pl.multiple_of(core * TOKENS, TOKENS), TOKENS), :]
        other = r3[b]
        left = jnp.where(core == 0, mine, other)
        right = jnp.where(core == 0, other, mine)
        rows = slice(b * TOKENS, (b + 1) * TOKENS)
        yv[b, :, :HALF] = (hv[rows, :HALF].astype(F32) + left).astype(BF16)
        yv[b, :, HALF:] = (hv[rows, HALF:].astype(F32) + right).astype(BF16)
        copy = local(yv.at[b], out, sem_out.at[b])
        copy.start()
        return copy

    relay(0)
    relay_far(0)
    gathered(0)
    pick(0)
    relay(1)
    experts(0)
    relay_far(1)
    o_wait(0)
    combine(0)
    far_copy(0).start()
    near_copy(0).start()
    gathered(1)
    pick(1)
    experts(1)
    fold(0)
    o_wait(1)
    combine(1)
    far_copy(1).start()
    near_copy(1).start()
    finish(0)
    fold(1)
    done_a = write_out(0, out_a)
    finish(1)
    done_b = write_out(1, out_b)

    for k in range(1, GROUP):
        meta_copy(k).wait_send()
    for b in range(2):
        for make in (d_near_x, d_near_y, d_sib, d_fwd_x, d_fwd_y, d_sib_x, d_sib_y, d_sib_d, far_copy, near_copy, second_copy, last_copy):
            make(b).wait_send()
        for e in range(LOCAL):
            o_copy(b, e).wait_send()
    done_a.wait()
    done_b.wait()


def solution(mesh):
    row_spec = P(("dp", "ep"), None)
    full_spec = P(None, None, None)
    gain_spec = P(None)
    expert_spec = P("ep", None, None)
    in_specs = (row_spec,) * 8 + (gain_spec,) + (full_spec,) * 4 + (gain_spec,) + (expert_spec,) * 3

    any_spec = pl.BlockSpec(memory_space=pl.ANY)
    VM = pltpu.VMEM
    DMA = pltpu.SemaphoreType.DMA
    scratch = [
        VM((2 * TOKENS, DIM), BF16),
        VM((2, DIM // 128, 128), BF16),
        VM((2, SLOTS, TOKENS), jnp.int32),
        VM((2, SLOTS, TOKENS), jnp.int32),
        VM((2, SLOTS, TOKENS), BF16),
        VM((3, CHUNKS, CHUNK, DIM), BF16),
        VM((DIM, DIM), BF16),
        VM((LOCAL, DIM, FFN), BF16),
        VM((LOCAL, DIM, FFN), BF16),
        VM((LOCAL, FFN, DIM), BF16),
        VM((2 * TOKENS, DIM), BF16),
        VM((3, CHUNKS, 2 * TOKENS, CHUNK), BF16),
        VM((2 * TOKENS, DIM), BF16),
        VM((2 * TOKENS, DIM), BF16),
        VM((2, ROWS, DIM), BF16),
        VM((GROUP, 2, 2, SLOTS, 128), F32),
        VM((2, LROWS, ROWS), BF16),
        VM((2, 2 * LROWS, ROWS), BF16),
        VM((LROWS, DIM), BF16),
        VM((2, 2, 2 * LROWS, HALF), BF16),
        VM((2, ROWS, HALF), F32),
        VM((2, 2, 2 * TOKENS, HALF), F32),
        VM((2, 2 * TOKENS, HALF), F32),
        VM((2, 2 * TOKENS, HALF), F32),
        VM((2, 2 * TOKENS, HALF), F32),
        VM((2, TOKENS, HALF), F32),
        VM((2, TOKENS, DIM), BF16),
        DMA((10,)),
        DMA((3, CHUNKS)),
        DMA,
        DMA((3, LOCAL)),
        DMA((2,)),
        DMA((GROUP,)),
        DMA((GROUP,)),
        DMA((2, 8)),
        DMA((2, 8)),
        DMA((2, LOCAL)),
        DMA((2, LOCAL)),
        DMA((2, 4)),
        DMA((2, 4)),
    ]

    def device_fn(tokens_a, experts_a, slots_a, gates_a, tokens_b, experts_b, slots_b, gates_b, attn_gain, w_query, w_key, w_value, w_out, moe_gain, w_gate, w_up, w_down):
        def heads_first(w):
            return jnp.transpose(w, (1, 2, 0)).reshape(DIM, DIM)

        out = jax.ShapeDtypeStruct((TOKENS, DIM), BF16)
        return pl.pallas_call(
            kernel,
            out_shape=(out, out),
            in_specs=[any_spec] * 17,
            out_specs=(any_spec, any_spec),
            scratch_shapes=scratch,
            compiler_params=pltpu.CompilerParams(
                collective_id=0, has_side_effects=True, vmem_limit_bytes=66_000_000,
            ),
            name="moe_layer",
        )(
            tokens_a, experts_a.T, slots_a.T, gates_a.T, tokens_b, experts_b.T, slots_b.T, gates_b.T,
            attn_gain.reshape(DIM // 128, 128), heads_first(w_query), heads_first(w_key), heads_first(w_value),
            w_out.reshape(DIM, DIM), moe_gain.reshape(DIM // 128, 128), w_gate, w_up, w_down,
        )

    return jax.shard_map(device_fn, mesh=mesh, in_specs=in_specs, out_specs=(row_spec, row_spec), check_vma=False)
```

```python
import functools

import jax
import jax.numpy as jnp
from jax import lax
from jax.experimental import pallas as pl
from jax.experimental.pallas import tpu as pltpu
from jax.sharding import PartitionSpec as P

NORM_EPS = 1e-6
MASK_VALUE = -1e30
MESH = pl.DeviceIdType.MESH

GROUP = 8
TOKENS = 32
DIM = 1536
FFN = 512
LOCAL = 5
SLOTS = 8
HALF = DIM // 2
CHUNK = 256
CHUNKS = DIM // CHUNK
BLOCKS = ((0, 1), (1, 2), (2, 4), (4, 6))
ROWS = GROUP * TOKENS
LROWS = LOCAL * GROUP * SLOTS
F32 = jnp.float32
BF16 = jnp.bfloat16

NT = (((1,), (1,)), ((), ()))
TN = (((0,), (0,)), ((), ()))


def twice(x):
    return jnp.concatenate([x, x], axis=0)


def rms_rows(rows_f, gain):
    inv = lax.rsqrt(jnp.mean(rows_f * rows_f, axis=-1, keepdims=True) + NORM_EPS)
    return (rows_f * inv * gain).astype(BF16)


def kernel(
    tok_a, exp_a, slot_a, gate_a, tok_b, exp_b, slot_b, gate_b,
    again_hbm, wq_hbm, wk_hbm, wv_hbm, wo_hbm, mgain_hbm, wg_hbm, wu_hbm, wd_hbm,
    out_y,
    xv, gains, ev, sv, gv,
    wqkv, wov, wgv, wuv, wdv,
    norm_a, qkv, ctx, hv, uall, meta, disp, comb, picked, o2, part, r1, s2, r2, fin, r3,
    sem_in, sem_qkv, sem_o, sem_exp,
    msend, mrecv, dsend, drecv, osend, orecv, rsend, rrecv,
):
    me = lax.axis_index("ep")
    core = me % 2
    px = (me // 2) % 2
    py = me // 4
    flip1 = me + 1 - 2 * core
    flip2 = me + 2 - 4 * px
    flip4 = me + 4 - 8 * py
    flip = {
        1: flip1,
        2: flip2,
        4: flip4,
        3: flip2 + 1 - 2 * core,
        5: flip4 + 1 - 2 * core,
        6: flip2 + 4 - 8 * py,
    }
    flip[7] = flip[6] + 1 - 2 * core
    first = (1 - core) * flip2 + core * flip4
    second = (1 - core) * flip4 + core * flip2

    def local(src, dst, sem):
        return pltpu.make_async_copy(src, dst, sem)

    def remote(src, dst, ssem, rsem, dev):
        return pltpu.make_async_remote_copy(
            src_ref=src, dst_ref=dst, send_sem=ssem, recv_sem=rsem,
            device_id={"ep": dev}, device_id_type=MESH,
        )

    small = [
        local(exp_a, ev.at[0], sem_in.at[0]),
        local(exp_b, ev.at[1], sem_in.at[1]),
        local(slot_a, sv.at[0], sem_in.at[2]),
        local(slot_b, sv.at[1], sem_in.at[3]),
        local(gate_a, gv.at[0], sem_in.at[4]),
        local(gate_b, gv.at[1], sem_in.at[5]),
        local(tok_a, xv.at[pl.ds(0, TOKENS)], sem_in.at[6]),
        local(tok_b, xv.at[pl.ds(TOKENS, TOKENS)], sem_in.at[7]),
        local(again_hbm, gains.at[0], sem_in.at[8]),
        local(mgain_hbm, gains.at[1], sem_in.at[9]),
    ]
    for copy in small:
        copy.start()

    whbm = (wq_hbm, wk_hbm, wv_hbm)

    def qkv_copy(which, c):
        rows = pl.ds(pl.multiple_of(c * CHUNK, CHUNK), CHUNK)
        return local(whbm[which].at[rows], wqkv.at[which, rows], sem_qkv.at[which, c])

    for which in range(3):
        qkv_copy(which, 0).start()
    wo_copy = local(wo_hbm, wov, sem_o)

    barrier = pltpu.get_barrier_semaphore()
    for k in range(1, GROUP):
        pl.semaphore_signal(barrier, inc=1, device_id={"ep": flip[k]}, device_id_type=MESH)

    for copy in small:
        copy.wait()
    for c in range(1, CHUNKS):
        for which in range(3):
            qkv_copy(which, c).start()
    wo_copy.start()

    def gain_row(i):
        g = gains[i].astype(F32)
        return jnp.concatenate([g[j:j + 1] for j in range(DIM // 128)], axis=1)

    norm_a[...] = rms_rows(xv[...].astype(F32), gain_row(0))

    lane = lax.broadcasted_iota(jnp.int32, (SLOTS, 128), 1)
    my_lanes = lane // TOKENS == me % 4
    for b in range(2):
        code = jnp.where(sv[b] >= 0, ev[b] * SLOTS + sv[b], -1).astype(F32)
        code = jnp.concatenate([code] * 4, axis=1)
        gate = jnp.concatenate([gv[b].astype(F32)] * 4, axis=1)
        meta[me, b, 0] = jnp.where(my_lanes, code, -1.0)
        meta[me, b, 1] = jnp.where(my_lanes, gate, 0.0)

    pl.semaphore_wait(barrier, GROUP - 1)

    def meta_copy(k):
        return remote(meta.at[me], meta.at[me], msend.at[k], mrecv.at[k], flip[k])

    for k in range(1, GROUP):
        meta_copy(k).start()


    n2 = 2 * TOKENS
    lane128 = lax.broadcasted_iota(jnp.int32, (n2, 128), 1)
    row128 = lax.broadcasted_iota(jnp.int32, (n2, 128), 0)
    key = lane128 % n2
    visible = (key // TOKENS == row128 // TOKENS) & (key <= row128)
    low = lane128 < n2
    head_of = lax.broadcasted_iota(jnp.int32, (n2, CHUNK), 1) // n2
    scale = 64.0 ** -0.5

    def softmax_pair(s):
        s = jnp.where(visible, s * scale, MASK_VALUE)
        m0 = jnp.max(jnp.where(low, s, -jnp.inf), axis=-1, keepdims=True)
        m1 = jnp.max(jnp.where(low, -jnp.inf, s), axis=-1, keepdims=True)
        p = jnp.exp(s - jnp.where(low, m0, m1))
        d0 = jnp.sum(jnp.where(low, p, 0.0), axis=-1, keepdims=True)
        d1 = jnp.sum(jnp.where(low, 0.0, p), axis=-1, keepdims=True)
        return (p / jnp.where(low, d0, d1)).astype(BF16)

    def spread(x):
        zero = jnp.zeros_like(x)
        return jnp.concatenate([jnp.where(head_of == g, x, zero) for g in range(CHUNK // n2)], axis=0)

    def lanes(which, c):
        return qkv[which, :, c * CHUNK:(c + 1) * CHUNK]

    def project(which, lo, hi):
        cols = slice(lo * CHUNK, hi * CHUNK)
        prod = lax.dot_general(norm_a[...], wqkv[which, cols, :], NT, preferred_element_type=F32)
        qkv[which, :, cols] = prod.astype(BF16)

    def scores(c):
        return lax.dot_general(lanes(0, c), spread(lanes(1, c)), NT, preferred_element_type=F32)

    def softmax(s):
        return jnp.concatenate([softmax_pair(s[:, i * 128:(i + 1) * 128]) for i in range(CHUNK // 128)], axis=1)

    def store_context(c, p):
        ctx[:, c * CHUNK:(c + 1) * CHUNK] = jnp.dot(p, spread(lanes(2, c)), preferred_element_type=F32).astype(BF16)

    before = ()
    for lo, hi in BLOCKS:
        for c in range(lo, hi):
            for which in range(3):
                qkv_copy(which, c).wait()
        raw = [scores(c) for c in before]
        project(0, lo, hi)
        probs = [softmax(s) for s in raw]
        project(1, lo, hi)
        for c, p in zip(before, probs):
            store_context(c, p)
        project(2, lo, hi)
        before = tuple(range(lo, hi))

    def expert_copies(e):
        return (
            local(wg_hbm.at[e], wgv.at[e], sem_exp.at[0, e]),
            local(wu_hbm.at[e], wuv.at[e], sem_exp.at[1, e]),
            local(wd_hbm.at[e], wdv.at[e], sem_exp.at[2, e]),
        )

    for e in range(LOCAL):
        for copy in expert_copies(e):
            copy.start()

    raw = [scores(c) for c in before]
    probs = [softmax(s) for s in raw]
    for c, p in zip(before, probs):
        store_context(c, p)

    wo_copy.wait()
    attn = jnp.dot(twice(ctx[...]), wov[...], preferred_element_type=F32)[:n2]
    h = (xv[...].astype(F32) + attn).astype(BF16)
    hv[...] = h
    u = rms_rows(h.astype(F32), gain_row(1))
    my_rows = pl.ds(pl.multiple_of(me * TOKENS, TOKENS), TOKENS)
    uall[0, my_rows, :] = u[:TOKENS]
    uall[1, my_rows, :] = u[TOKENS:]

    def block(b, dev, lo=0, n=TOKENS):
        return uall.at[b, pl.ds(pl.multiple_of(dev * TOKENS + lo, 16), n)]

    def disp_copy(b, i, dev_block, target, slot, lo=0, n=TOKENS):
        ref = block(b, dev_block, lo, n)
        return remote(ref, ref, dsend.at[b, i], drecv.at[b, slot], target)

    H = TOKENS // 2

    def d_x(b, part):
        return disp_copy(b, part, me, flip[2], part, part * H, H)

    def d_y(b, part):
        return disp_copy(b, 2 + part, me, flip[4], 2 + part, part * H, H)

    def d_sib(b):
        return disp_copy(b, 6, me, flip[1], 6)

    def d_fwd_x(b):
        return disp_copy(b, 4, flip[2], flip[4], 4, 0, H)

    def d_fwd_y(b):
        return disp_copy(b, 5, flip[4], flip[2], 5, H, H)

    def d_sib_x(b):
        return disp_copy(b, 7, flip[2], flip[1], 7)

    def d_sib_y(b):
        return disp_copy(b, 8, flip[4], flip[1], 8)

    def d_sib_d(b):
        return disp_copy(b, 9, flip[6], flip[1], 9)

    def d_wait(b, slot, dev, lo=0, n=TOKENS):
        ref = block(b, dev, lo, n)
        remote(ref, ref, dsend.at[b, 0], drecv.at[b, slot], flip[1]).wait_recv()

    def send_own(b):
        d_x(b, 0).start()
        d_y(b, 1).start()
        d_x(b, 1).start()
        d_y(b, 0).start()
        d_sib(b).start()

    send_own(0)

    for k in range(1, GROUP):
        remote(meta.at[flip[k]], meta.at[flip[k]], msend.at[k], mrecv.at[k], flip[k]).wait_recv()

    slot_row = lax.broadcasted_iota(jnp.int32, (SLOTS, ROWS), 0)
    row64 = lax.broadcasted_iota(jnp.int32, (GROUP * SLOTS, ROWS), 0)
    lane64 = lax.broadcasted_iota(jnp.int32, (GROUP * SLOTS, ROWS), 1)
    owner_hit = lane64 // TOKENS == row64 // SLOTS
    for b in range(2):
        halves = []
        for kind in range(2):
            parts = []
            for side in range(2):
                acc = meta[4 * side, b, kind]
                for p in range(1, 4):
                    acc = jnp.maximum(acc, meta[4 * side + p, b, kind])
                parts.append(acc)
            halves.append(jnp.concatenate(parts, axis=1))
        code, gate = halves
        code_rows = [jnp.broadcast_to(code[j:j + 1], (SLOTS, ROWS)) for j in range(SLOTS)]
        gate_rows = [jnp.broadcast_to(gate[j:j + 1], (SLOTS, ROWS)) for j in range(SLOTS)]
        for who in range(2):
            dev = me if who == 0 else flip[1]
            for e in range(LOCAL):
                target = ((dev * LOCAL + e) * SLOTS + slot_row).astype(F32)
                hit = jnp.zeros((SLOTS, ROWS), F32)
                weight = jnp.zeros((SLOTS, ROWS), F32)
                for j in range(SLOTS):
                    match = code_rows[j] == target
                    weight = weight + jnp.where(match, gate_rows[j], 0.0)
                    if who == 0:
                        hit = hit + jnp.where(match, 1.0, 0.0)
                rows = slice((who * LOCAL + e) * 64, (who * LOCAL + e + 1) * 64)
                wide = jnp.concatenate([weight] * GROUP, axis=0)
                comb[b, rows, :] = jnp.where(owner_hit, wide, 0.0).astype(BF16)
                if who == 0:
                    wide = jnp.concatenate([hit] * GROUP, axis=0)
                    disp[b, e * 64:(e + 1) * 64, :] = jnp.where(owner_hit, wide, 0.0).astype(BF16)

    def relay(b):
        d_wait(b, 0, flip[2], 0, H)
        d_fwd_x(b).start()
        d_wait(b, 3, flip[4], H, H)
        d_fwd_y(b).start()

    def relay_near(b):
        d_wait(b, 1, flip[2], H, H)
        d_sib_x(b).start()
        d_wait(b, 2, flip[4], 0, H)
        d_sib_y(b).start()

    def relay_far(b):
        d_wait(b, 4, flip[6], 0, H)
        d_wait(b, 5, flip[6], H, H)
        d_sib_d(b).start()

    def gathered(b):
        d_wait(b, 6, flip[1])
        d_wait(b, 7, flip[3])
        d_wait(b, 8, flip[5])
        d_wait(b, 9, flip[7])

    def pick(b):
        for n in range(CHUNKS):
            cols = slice(n * CHUNK, (n + 1) * CHUNK)
            picked[:, cols] = jnp.dot(disp[b], uall[b, :, cols], preferred_element_type=F32).astype(BF16)

    def o_copy(b, e):
        src = o2.at[b, 1 - core, pl.ds(e * 64, 64)]
        dst = o2.at[b, 1 - core, pl.ds(LROWS + e * 64, 64)]
        return remote(src, dst, osend.at[b, e], orecv.at[b, e], flip[1])

    def o_wait(b):
        for e in range(LOCAL):
            ref = o2.at[b, core, pl.ds(LROWS + e * 64, 64)]
            remote(ref, ref, osend.at[b, e], orecv.at[b, e], flip[1]).wait_recv()

    def gate_up(e):
        x = twice(picked[e * 64:(e + 1) * 64, :])
        g = jnp.dot(x, wgv[e], preferred_element_type=F32)
        up = jnp.dot(x, wuv[e], preferred_element_type=F32)
        return g[:64], up[:64]

    def experts(b):
        if b == 0:
            for e in range(LOCAL):
                for copy in expert_copies(e):
                    copy.wait()
        g, up = gate_up(0)
        for e in range(LOCAL):
            hidden = (g * (1.0 / (1.0 + jnp.exp(-g))) * up).astype(BF16)
            if e + 1 < LOCAL:
                g, up = gate_up(e + 1)
            o = jnp.dot(twice(hidden), wdv[e], preferred_element_type=F32)[:64].astype(BF16)
            rows = slice(e * 64, (e + 1) * 64)
            o2[b, 0, rows, :] = o[:, :HALF]
            o2[b, 1, rows, :] = o[:, HALF:]
            if e > 0:
                o_copy(b, e - 1).start()
        o_copy(b, LOCAL - 1).start()

    def combine(b):
        for n in range(HALF // CHUNK):
            cols = slice(n * CHUNK, (n + 1) * CHUNK)
            part[b, :, cols] = lax.dot_general(comb[b], o2[b, core, :, cols], TN, preferred_element_type=F32)

    def chip_rows(ref, b, dev):
        return ref.at[b, pl.ds(pl.multiple_of((dev // 2) * 64, 64), 64)]

    def far_copy(b):
        return remote(chip_rows(part, b, flip[6]), r1.at[b, 1], rsend.at[b, 0], rrecv.at[b, 0], first)

    def near_copy(b):
        return remote(chip_rows(part, b, first), r1.at[b, 0], rsend.at[b, 1], rrecv.at[b, 1], first)

    def second_copy(b):
        return remote(s2.at[b], r2.at[b], rsend.at[b, 2], rrecv.at[b, 2], second)

    def last_copy(b):
        rows = pl.ds(pl.multiple_of((1 - core) * TOKENS, TOKENS), TOKENS)
        return remote(fin.at[b, rows], r3.at[b], rsend.at[b, 3], rrecv.at[b, 3], flip[1])

    def wide_rows(dev):
        return pl.ds(pl.multiple_of((dev // 2) * 64, 64), 64)

    def fold(b):
        far_copy(b).wait_recv()
        s2[b] = part[b, wide_rows(second), :] + r1[b, 1]
        second_copy(b).start()

    def finish(b):
        near_copy(b).wait_recv()
        second_copy(b).wait_recv()
        fin[b] = part[b, wide_rows(me), :] + r1[b, 0] + r2[b]
        last_copy(b).start()

    def write_out(b, out):
        last_copy(b).wait_recv()
        mine = fin[b, pl.ds(pl.multiple_of(core * TOKENS, TOKENS), TOKENS), :]
        other = r3[b]
        left = jnp.where(core == 0, mine, other)
        right = jnp.where(core == 0, other, mine)
        rows = slice(b * TOKENS, (b + 1) * TOKENS)
        out[:, :HALF] = (hv[rows, :HALF].astype(F32) + left).astype(BF16)
        out[:, HALF:] = (hv[rows, HALF:].astype(F32) + right).astype(BF16)

    relay(0)
    send_own(1)
    relay_near(0)
    relay_far(0)
    gathered(0)
    pick(0)
    relay(1)
    relay_near(1)
    experts(0)
    relay_far(1)
    o_wait(0)
    combine(0)
    far_copy(0).start()
    near_copy(0).start()
    gathered(1)
    pick(1)
    experts(1)
    fold(0)
    o_wait(1)
    combine(1)
    far_copy(1).start()
    near_copy(1).start()
    finish(0)
    fold(1)
    write_out(0, out_y.at[0])
    finish(1)
    write_out(1, out_y.at[1])

    for k in range(1, GROUP):
        meta_copy(k).wait_send()
    for b in range(2):
        for part_id in range(2):
            d_x(b, part_id).wait_send()
            d_y(b, part_id).wait_send()
        for make in (d_sib, d_fwd_x, d_fwd_y, d_sib_x, d_sib_y, d_sib_d, far_copy, near_copy, second_copy, last_copy):
            make(b).wait_send()
        for e in range(LOCAL):
            o_copy(b, e).wait_send()


def solution(mesh):
    row_spec = P(("dp", "ep"), None)
    full_spec = P(None, None, None)
    gain_spec = P(None)
    expert_spec = P("ep", None, None)
    in_specs = (row_spec,) * 8 + (gain_spec,) + (full_spec,) * 4 + (gain_spec,) + (expert_spec,) * 3

    hbm_spec = pl.BlockSpec(memory_space=pltpu.HBM)
    VM = pltpu.VMEM
    DMA = pltpu.SemaphoreType.DMA
    scratch = [
        VM((2 * TOKENS, DIM), BF16),
        VM((2, DIM // 128, 128), BF16),
        VM((2, SLOTS, TOKENS), jnp.int32),
        VM((2, SLOTS, TOKENS), jnp.int32),
        VM((2, SLOTS, TOKENS), BF16),
        VM((3, DIM, DIM), BF16),
        VM((DIM, DIM), BF16),
        VM((LOCAL, DIM, FFN), BF16),
        VM((LOCAL, DIM, FFN), BF16),
        VM((LOCAL, FFN, DIM), BF16),
        VM((2 * TOKENS, DIM), BF16),
        VM((3, 2 * TOKENS, DIM), BF16),
        VM((2 * TOKENS, DIM), BF16),
        VM((2 * TOKENS, DIM), BF16),
        VM((2, ROWS, DIM), BF16),
        VM((GROUP, 2, 2, SLOTS, 128), F32),
        VM((2, LROWS, ROWS), BF16),
        VM((2, 2 * LROWS, ROWS), BF16),
        VM((LROWS, DIM), BF16),
        VM((2, 2, 2 * LROWS, HALF), BF16),
        VM((2, ROWS, HALF), F32),
        VM((2, 2, 2 * TOKENS, HALF), F32),
        VM((2, 2 * TOKENS, HALF), F32),
        VM((2, 2 * TOKENS, HALF), F32),
        VM((2, 2 * TOKENS, HALF), F32),
        VM((2, TOKENS, HALF), F32),
        DMA((10,)),
        DMA((3, CHUNKS)),
        DMA,
        DMA((3, LOCAL)),
        DMA((GROUP,)),
        DMA((GROUP,)),
        DMA((2, 10)),
        DMA((2, 10)),
        DMA((2, LOCAL)),
        DMA((2, LOCAL)),
        DMA((2, 4)),
        DMA((2, 4)),
    ]

    def device_fn(tokens_a, experts_a, slots_a, gates_a, tokens_b, experts_b, slots_b, gates_b, attn_gain, w_query, w_key, w_value, w_out, moe_gain, w_gate, w_up, w_down):
        def heads_first(w):
            return jnp.transpose(w, (1, 2, 0)).reshape(DIM, DIM)

        out = VM((2, TOKENS, DIM), BF16)
        y = pl.pallas_call(
            kernel,
            out_shape=out,
            in_specs=[hbm_spec] * 17,
            out_specs=pl.BlockSpec(memory_space=pltpu.VMEM),
            scratch_shapes=scratch,
            compiler_params=pltpu.CompilerParams(
                collective_id=0, has_side_effects=True, vmem_limit_bytes=58000000,
            ),
            name="moe_layer",
        )(
            tokens_a, experts_a.T, slots_a.T, gates_a.T, tokens_b, experts_b.T, slots_b.T, gates_b.T,
            attn_gain.reshape(DIM // 128, 128), heads_first(w_query), heads_first(w_key), heads_first(w_value),
            w_out.reshape(DIM, DIM), moe_gain.reshape(DIM // 128, 128), w_gate, w_up, w_down,
        )
        return y[0], y[1]

    return jax.shard_map(device_fn, mesh=mesh, in_specs=in_specs, out_specs=(row_spec, row_spec), check_vma=False)
```

```python
import functools

import jax
import jax.numpy as jnp
from jax import lax
from jax.experimental import pallas as pl
from jax.experimental.pallas import tpu as pltpu
from jax.sharding import PartitionSpec as P

NORM_EPS = 1e-6
MASK_VALUE = -1e30
MESH = pl.DeviceIdType.MESH

GROUP = 8
TOKENS = 32
DIM = 1536
FFN = 512
LOCAL = 5
SLOTS = 8
HALF = DIM // 2
CHUNK = 256
CHUNKS = DIM // CHUNK
PIECES = HALF // CHUNK
FLIPPED = (1, 2)
ROWS = GROUP * TOKENS
LROWS = LOCAL * GROUP * SLOTS
F32 = jnp.float32
BF16 = jnp.bfloat16

NT = (((1,), (1,)), ((), ()))
TN = (((0,), (0,)), ((), ()))


def twice(x):
    return jnp.concatenate([x, x], axis=0)


def rms_rows(rows_f, gain):
    inv = lax.rsqrt(jnp.mean(rows_f * rows_f, axis=-1, keepdims=True) + NORM_EPS)
    return (rows_f * inv * gain).astype(BF16)


def kernel(
    tok_a, exp_a, slot_a, gate_a, tok_b, exp_b, slot_b, gate_b,
    again_hbm, wq_hbm, wk_hbm, wv_hbm, wo_hbm, mgain_hbm, wg_hbm, wu_hbm, wd_hbm,
    out_y,
    xv, gains, ev, sv, gv,
    wqkv, wov, wgv, wuv, wdv,
    wt, norm_a, qkv, ctx, hv, uall, meta, disp, comb, combt, picked, hidden, o2, part, r1, s2, r2, fin, r3,
    sem_in, sem_qkv, sem_o, sem_exp,
    msend, mrecv, dsend, drecv, osend, orecv, rsend, rrecv,
):
    me = lax.axis_index("ep")
    core = me % 2
    px = (me // 2) % 2
    py = me // 4
    flip1 = me + 1 - 2 * core
    flip2 = me + 2 - 4 * px
    flip4 = me + 4 - 8 * py
    flip = {
        1: flip1,
        2: flip2,
        4: flip4,
        3: flip2 + 1 - 2 * core,
        5: flip4 + 1 - 2 * core,
        6: flip2 + 4 - 8 * py,
    }
    flip[7] = flip[6] + 1 - 2 * core
    first = (1 - core) * flip2 + core * flip4
    second = (1 - core) * flip4 + core * flip2

    def local(src, dst, sem):
        return pltpu.make_async_copy(src, dst, sem)

    def remote(src, dst, ssem, rsem, dev):
        return pltpu.make_async_remote_copy(
            src_ref=src, dst_ref=dst, send_sem=ssem, recv_sem=rsem,
            device_id={"ep": dev}, device_id_type=MESH,
        )

    small = [
        local(exp_a, ev.at[0], sem_in.at[0]),
        local(exp_b, ev.at[1], sem_in.at[1]),
        local(slot_a, sv.at[0], sem_in.at[2]),
        local(slot_b, sv.at[1], sem_in.at[3]),
        local(gate_a, gv.at[0], sem_in.at[4]),
        local(gate_b, gv.at[1], sem_in.at[5]),
        local(tok_a, xv.at[pl.ds(0, TOKENS)], sem_in.at[6]),
        local(tok_b, xv.at[pl.ds(TOKENS, TOKENS)], sem_in.at[7]),
        local(again_hbm, gains.at[0], sem_in.at[8]),
        local(mgain_hbm, gains.at[1], sem_in.at[9]),
    ]
    for copy in small:
        copy.start()

    whbm = (wq_hbm, wk_hbm, wv_hbm)

    def qkv_copy(which, c):
        rows = pl.ds(pl.multiple_of(c * CHUNK, CHUNK), CHUNK)
        return local(whbm[which].at[rows], wqkv.at[which, rows], sem_qkv.at[which, c])

    for which in range(3):
        qkv_copy(which, 0).start()
    wo_copy = local(wo_hbm, wov, sem_o)

    barrier = pltpu.get_barrier_semaphore()
    for k in range(1, GROUP):
        pl.semaphore_signal(barrier, inc=1, device_id={"ep": flip[k]}, device_id_type=MESH)

    small[0].wait()
    for which in range(3):
        qkv_copy(which, 1).start()
    for copy in small[1:]:
        copy.wait()
    for c in range(2, CHUNKS):
        for which in range(3):
            qkv_copy(which, c).start()
    wo_copy.start()

    def gain_row(i):
        g = gains[i].astype(F32)
        return jnp.concatenate([g[j:j + 1] for j in range(DIM // 128)], axis=1)

    norm_a[...] = rms_rows(xv[...].astype(F32), gain_row(0))

    lane = lax.broadcasted_iota(jnp.int32, (SLOTS, 128), 1)
    my_lanes = lane // TOKENS == me % 4
    for b in range(2):
        code = jnp.where(sv[b] >= 0, ev[b] * SLOTS + sv[b], -1).astype(F32)
        code = jnp.concatenate([code] * 4, axis=1)
        gate = jnp.concatenate([gv[b].astype(F32)] * 4, axis=1)
        meta[me, b, 0] = jnp.where(my_lanes, code, -1.0)
        meta[me, b, 1] = jnp.where(my_lanes, gate, 0.0)

    pl.semaphore_wait(barrier, GROUP - 1)

    def meta_copy(k):
        return remote(meta.at[me], meta.at[me], msend.at[k], mrecv.at[k], flip[k])

    for k in range(1, GROUP):
        meta_copy(k).start()


    n2 = 2 * TOKENS
    lane128 = lax.broadcasted_iota(jnp.int32, (n2, 128), 1)
    row128 = lax.broadcasted_iota(jnp.int32, (n2, 128), 0)
    key = lane128 % n2
    visible = (key // TOKENS == row128 // TOKENS) & (key <= row128)
    low = lane128 < n2
    head_of = lax.broadcasted_iota(jnp.int32, (n2, CHUNK), 1) // n2
    scale = 64.0 ** -0.5

    def softmax_pair(s):
        s = jnp.where(visible, s * scale, MASK_VALUE)
        m0 = jnp.max(jnp.where(low, s, -jnp.inf), axis=-1, keepdims=True)
        m1 = jnp.max(jnp.where(low, -jnp.inf, s), axis=-1, keepdims=True)
        p = jnp.exp(s - jnp.where(low, m0, m1))
        d0 = jnp.sum(jnp.where(low, p, 0.0), axis=-1, keepdims=True)
        d1 = jnp.sum(jnp.where(low, 0.0, p), axis=-1, keepdims=True)
        return (p / jnp.where(low, d0, d1)).astype(BF16)

    def spread(x):
        zero = jnp.zeros_like(x)
        return jnp.concatenate([jnp.where(head_of == g, x, zero) for g in range(CHUNK // n2)], axis=0)

    def lanes(which, c):
        return qkv[which, :, c * CHUNK:(c + 1) * CHUNK]

    def project(which, c):
        cols = slice(c * CHUNK, (c + 1) * CHUNK)
        if which in FLIPPED:
            wt[...] = wqkv[which, cols, :].T
            prod = jnp.dot(twice(norm_a[...]), wt[...], preferred_element_type=F32)[:n2]
        else:
            prod = lax.dot_general(norm_a[...], wqkv[which, cols, :], NT, preferred_element_type=F32)
        qkv[which, :, cols] = prod.astype(BF16)

    def scores(c):
        return lax.dot_general(lanes(0, c), spread(lanes(1, c)), NT, preferred_element_type=F32)

    def softmax(s):
        return jnp.concatenate([softmax_pair(s[:, i * 128:(i + 1) * 128]) for i in range(CHUNK // 128)], axis=1)

    def store_context(c, p):
        ctx[:, c * CHUNK:(c + 1) * CHUNK] = jnp.dot(p, spread(lanes(2, c)), preferred_element_type=F32).astype(BF16)

    for c in range(CHUNKS):
        for which in range(3):
            qkv_copy(which, c).wait()
        raw = scores(c - 1) if c else None
        project(0, c)
        probs = softmax(raw) if c else None
        project(1, c)
        if c:
            store_context(c - 1, probs)
        project(2, c)

    def expert_copy(which, e):
        hbm, vmem = ((wg_hbm, wgv), (wu_hbm, wuv), (wd_hbm, wdv))[which]
        return local(hbm.at[e], vmem.at[e], sem_exp.at[which, e])

    for e in range(LOCAL):
        for which in range(3):
            expert_copy(which, e).start()

    store_context(CHUNKS - 1, softmax(scores(CHUNKS - 1)))

    wo_copy.wait()
    attn = jnp.dot(twice(ctx[...]), wov[...], preferred_element_type=F32)[:n2]
    h = (xv[...].astype(F32) + attn).astype(BF16)
    hv[...] = h
    u = rms_rows(h.astype(F32), gain_row(1))
    my_rows = pl.ds(pl.multiple_of(me * TOKENS, TOKENS), TOKENS)
    uall[0, my_rows, :] = u[:TOKENS]
    uall[1, my_rows, :] = u[TOKENS:]

    def block(b, dev, lo=0, n=TOKENS):
        return uall.at[b, pl.ds(pl.multiple_of(dev * TOKENS + lo, 16), n)]

    def disp_copy(b, i, dev_block, target, slot, lo=0, n=TOKENS):
        ref = block(b, dev_block, lo, n)
        return remote(ref, ref, dsend.at[b, i], drecv.at[b, slot], target)

    H = TOKENS // 2

    def d_x(b, part):
        return disp_copy(b, part, me, flip[2], part, part * H, H)

    def d_y(b, part):
        return disp_copy(b, 2 + part, me, flip[4], 2 + part, part * H, H)

    def d_sib(b):
        return disp_copy(b, 6, me, flip[1], 6)

    def d_fwd_x(b):
        return disp_copy(b, 4, flip[2], flip[4], 4, 0, H)

    def d_fwd_y(b):
        return disp_copy(b, 5, flip[4], flip[2], 5, H, H)

    def d_sib_x(b):
        return disp_copy(b, 7, flip[2], flip[1], 7)

    def d_sib_y(b):
        return disp_copy(b, 8, flip[4], flip[1], 8)

    def d_sib_d(b):
        return disp_copy(b, 9, flip[6], flip[1], 9)

    def d_wait(b, slot, dev, lo=0, n=TOKENS):
        ref = block(b, dev, lo, n)
        remote(ref, ref, dsend.at[b, 0], drecv.at[b, slot], flip[1]).wait_recv()

    def send_own(b):
        d_x(b, 0).start()
        d_y(b, 1).start()
        d_x(b, 1).start()
        d_y(b, 0).start()
        d_sib(b).start()

    send_own(0)

    for k in range(1, GROUP):
        remote(meta.at[flip[k]], meta.at[flip[k]], msend.at[k], mrecv.at[k], flip[k]).wait_recv()

    slot_row = lax.broadcasted_iota(jnp.int32, (SLOTS, ROWS), 0)
    row64 = lax.broadcasted_iota(jnp.int32, (GROUP * SLOTS, ROWS), 0)
    lane64 = lax.broadcasted_iota(jnp.int32, (GROUP * SLOTS, ROWS), 1)
    owner_hit = lane64 // TOKENS == row64 // SLOTS
    for b in range(2):
        halves = []
        for kind in range(2):
            parts = []
            for side in range(2):
                acc = meta[4 * side, b, kind]
                for p in range(1, 4):
                    acc = jnp.maximum(acc, meta[4 * side + p, b, kind])
                parts.append(acc)
            halves.append(jnp.concatenate(parts, axis=1))
        code, gate = halves
        code_rows = [jnp.broadcast_to(code[j:j + 1], (SLOTS, ROWS)) for j in range(SLOTS)]
        gate_rows = [jnp.broadcast_to(gate[j:j + 1], (SLOTS, ROWS)) for j in range(SLOTS)]
        for who in range(2):
            dev = me if who == 0 else flip[1]
            for e in range(LOCAL):
                target = ((dev * LOCAL + e) * SLOTS + slot_row).astype(F32)
                hit = jnp.zeros((SLOTS, ROWS), F32)
                weight = jnp.zeros((SLOTS, ROWS), F32)
                for j in range(SLOTS):
                    match = code_rows[j] == target
                    weight = weight + jnp.where(match, gate_rows[j], 0.0)
                    if who == 0:
                        hit = hit + jnp.where(match, 1.0, 0.0)
                rows = slice((who * LOCAL + e) * 64, (who * LOCAL + e + 1) * 64)
                wide = jnp.concatenate([weight] * GROUP, axis=0)
                comb[b, rows, :] = jnp.where(owner_hit, wide, 0.0).astype(BF16)
                if who == 0:
                    wide = jnp.concatenate([hit] * GROUP, axis=0)
                    disp[b, e * 64:(e + 1) * 64, :] = jnp.where(owner_hit, wide, 0.0).astype(BF16)

    for b in range(2):
        combt[b] = comb[b].T

    def relay(b):
        d_wait(b, 0, flip[2], 0, H)
        d_fwd_x(b).start()
        d_wait(b, 3, flip[4], H, H)
        d_fwd_y(b).start()

    def relay_near(b):
        d_wait(b, 1, flip[2], H, H)
        d_sib_x(b).start()
        d_wait(b, 2, flip[4], 0, H)
        d_sib_y(b).start()

    def relay_far(b):
        d_wait(b, 4, flip[6], 0, H)
        d_wait(b, 5, flip[6], H, H)
        d_sib_d(b).start()

    def gathered(b):
        d_wait(b, 6, flip[1])
        d_wait(b, 7, flip[3])
        d_wait(b, 8, flip[5])
        d_wait(b, 9, flip[7])

    def pick(b):
        for n in range(CHUNKS):
            cols = slice(n * CHUNK, (n + 1) * CHUNK)
            picked[:, cols] = jnp.dot(disp[b], uall[b, :, cols], preferred_element_type=F32).astype(BF16)

    def gate_up(b, which):
        for e in which:
            if b == 0:
                expert_copy(0, e).wait()
                expert_copy(1, e).wait()
        for e in which:
            x = twice(picked[e * 64:(e + 1) * 64, :])
            g = jnp.dot(x, wgv[e], preferred_element_type=F32)[:64]
            up = jnp.dot(x, wuv[e], preferred_element_type=F32)[:64]
            hidden[e] = (g * (1.0 / (1.0 + jnp.exp(-g))) * up).astype(BF16)

    def wait_down():
        for e in range(LOCAL):
            expert_copy(2, e).wait()

    def o_copy(b, j):
        src = o2.at[b, 1 - core, j, pl.ds(0, LROWS)]
        dst = o2.at[b, 1 - core, j, pl.ds(LROWS, LROWS)]
        return remote(src, dst, osend.at[b, j], orecv.at[b, j], flip[1])

    def down(b, j):
        for e in range(LOCAL):
            x = twice(hidden[e])
            for side in range(2):
                cols = slice(side * HALF + j * CHUNK, side * HALF + (j + 1) * CHUNK)
                o = jnp.dot(x, wdv[e, :, cols], preferred_element_type=F32)[:64]
                o2[b, side, j, e * 64:(e + 1) * 64, :] = o.astype(BF16)
        o_copy(b, j).start()

    def wide_rows(dev):
        return pl.ds(pl.multiple_of((dev // 2) * 64, 64), 64)

    def far_copy(b, j):
        return remote(part.at[b, j, wide_rows(flip[6])], r1.at[b, 1, j], rsend.at[b, 0, j], rrecv.at[b, 0, j], first)

    def near_copy(b, j):
        return remote(part.at[b, j, wide_rows(first)], r1.at[b, 0, j], rsend.at[b, 1, j], rrecv.at[b, 1, j], first)

    def second_copy(b, j):
        return remote(s2.at[b, j], r2.at[b, j], rsend.at[b, 2, j], rrecv.at[b, 2, j], second)

    def last_copy(b, j):
        rows = pl.ds(pl.multiple_of((1 - core) * TOKENS, TOKENS), TOKENS)
        return remote(fin.at[b, j, rows], r3.at[b, j], rsend.at[b, 3, j], rrecv.at[b, 3, j], flip[1])

    def combine(b, j):
        ref = o2.at[b, core, j, pl.ds(LROWS, LROWS)]
        remote(ref, ref, osend.at[b, j], orecv.at[b, j], flip[1]).wait_recv()
        part[b, j] = jnp.dot(combt[b], o2[b, core, j], preferred_element_type=F32)
        far_copy(b, j).start()

    def near_all(b):
        for j in range(PIECES):
            near_copy(b, j).start()

    def fold(b, j):
        far_copy(b, j).wait_recv()
        s2[b, j] = part[b, j, wide_rows(second), :] + r1[b, 1, j]
        second_copy(b, j).start()

    def finish(b, j):
        near_copy(b, j).wait_recv()
        second_copy(b, j).wait_recv()
        fin[b, j] = part[b, j, wide_rows(me), :] + r1[b, 0, j] + r2[b, j]
        last_copy(b, j).start()

    def write_out(b, j):
        last_copy(b, j).wait_recv()
        mine = fin[b, j, pl.ds(pl.multiple_of(core * TOKENS, TOKENS), TOKENS), :]
        other = r3[b, j]
        rows = slice(b * TOKENS, (b + 1) * TOKENS)
        for side in range(2):
            cols = slice(side * HALF + j * CHUNK, side * HALF + (j + 1) * CHUNK)
            mix = jnp.where(core == side, mine, other)
            out_y[b, :, cols] = (hv[rows, cols].astype(F32) + mix).astype(BF16)

    relay(0)
    send_own(1)
    relay_near(0)
    relay_far(0)
    gathered(0)
    pick(0)
    relay(1)
    gate_up(0, (0, 1))
    relay_near(1)
    gate_up(0, (2, 3, 4))
    wait_down()
    for j in range(PIECES): down(0, j)
    relay_far(1)
    for j in range(PIECES): combine(0, j)
    near_all(0)
    gathered(1)
    pick(1)
    gate_up(1, range(LOCAL))
    for j in range(PIECES): fold(0, j)
    for j in range(PIECES): down(1, j)
    for j in range(PIECES): combine(1, j)
    near_all(1)
    for j in range(PIECES): finish(0, j)
    for j in range(PIECES): fold(1, j)
    for j in range(PIECES): write_out(0, j)
    for j in range(PIECES): finish(1, j)
    for j in range(PIECES): write_out(1, j)

    for k in range(1, GROUP):
        meta_copy(k).wait_send()
    for b in range(2):
        for part_id in range(2):
            d_x(b, part_id).wait_send()
            d_y(b, part_id).wait_send()
        for make in (d_sib, d_fwd_x, d_fwd_y, d_sib_x, d_sib_y, d_sib_d):
            make(b).wait_send()
        for j in range(PIECES):
            for make in (o_copy, far_copy, near_copy, second_copy, last_copy):
                make(b, j).wait_send()


def solution(mesh):
    row_spec = P(("dp", "ep"), None)
    full_spec = P(None, None, None)
    gain_spec = P(None)
    expert_spec = P("ep", None, None)
    in_specs = (row_spec,) * 8 + (gain_spec,) + (full_spec,) * 4 + (gain_spec,) + (expert_spec,) * 3

    hbm_spec = pl.BlockSpec(memory_space=pltpu.HBM)
    VM = pltpu.VMEM
    DMA = pltpu.SemaphoreType.DMA
    scratch = [
        VM((2 * TOKENS, DIM), BF16),
        VM((2, DIM // 128, 128), BF16),
        VM((2, SLOTS, TOKENS), jnp.int32),
        VM((2, SLOTS, TOKENS), jnp.int32),
        VM((2, SLOTS, TOKENS), BF16),
        VM((3, DIM, DIM), BF16),
        VM((DIM, DIM), BF16),
        VM((LOCAL, DIM, FFN), BF16),
        VM((LOCAL, DIM, FFN), BF16),
        VM((LOCAL, FFN, DIM), BF16),
        VM((DIM, CHUNK), BF16),
        VM((2 * TOKENS, DIM), BF16),
        VM((3, 2 * TOKENS, DIM), BF16),
        VM((2 * TOKENS, DIM), BF16),
        VM((2 * TOKENS, DIM), BF16),
        VM((2, ROWS, DIM), BF16),
        VM((GROUP, 2, 2, SLOTS, 128), F32),
        VM((2, LROWS, ROWS), BF16),
        VM((2, 2 * LROWS, ROWS), BF16),
        VM((2, ROWS, 2 * LROWS), BF16),
        VM((LROWS, DIM), BF16),
        VM((LOCAL, 2 * TOKENS, FFN), BF16),
        VM((2, 2, PIECES, 2 * LROWS, CHUNK), BF16),
        VM((2, PIECES, ROWS, CHUNK), F32),
        VM((2, 2, PIECES, 2 * TOKENS, CHUNK), F32),
        VM((2, PIECES, 2 * TOKENS, CHUNK), F32),
        VM((2, PIECES, 2 * TOKENS, CHUNK), F32),
        VM((2, PIECES, 2 * TOKENS, CHUNK), F32),
        VM((2, PIECES, TOKENS, CHUNK), F32),
        DMA((10,)),
        DMA((3, CHUNKS)),
        DMA,
        DMA((3, LOCAL)),
        DMA((GROUP,)),
        DMA((GROUP,)),
        DMA((2, 10)),
        DMA((2, 10)),
        DMA((2, PIECES)),
        DMA((2, PIECES)),
        DMA((2, 4, PIECES)),
        DMA((2, 4, PIECES)),
    ]

    def device_fn(tokens_a, experts_a, slots_a, gates_a, tokens_b, experts_b, slots_b, gates_b, attn_gain, w_query, w_key, w_value, w_out, moe_gain, w_gate, w_up, w_down):
        def heads_first(w):
            return jnp.transpose(w, (1, 2, 0)).reshape(DIM, DIM)

        out = VM((2, TOKENS, DIM), BF16)
        y = pl.pallas_call(
            kernel,
            out_shape=out,
            in_specs=[hbm_spec] * 17,
            out_specs=pl.BlockSpec(memory_space=pltpu.VMEM),
            scratch_shapes=scratch,
            compiler_params=pltpu.CompilerParams(
                collective_id=0, has_side_effects=True, vmem_limit_bytes=58000000,
            ),
            name="moe_layer",
        )(
            tokens_a, experts_a.T, slots_a.T, gates_a.T, tokens_b, experts_b.T, slots_b.T, gates_b.T,
            attn_gain.reshape(DIM // 128, 128), heads_first(w_query), heads_first(w_key), heads_first(w_value),
            w_out.reshape(DIM, DIM), moe_gain.reshape(DIM // 128, 128), w_gate, w_up, w_down,
        )
        return y[0], y[1]

    return jax.shard_map(device_fn, mesh=mesh, in_specs=in_specs, out_specs=(row_spec, row_spec), check_vma=False)
```
